256 devices in a mesh: row: 16 (over y_lo, x, core), col: 16 (over z, y_hi).
Axes of the slice: x: 4, y: 4 (y_hi: 2, y_lo: 2; y = y_hi * 2 + y_lo), z: 8, core: 2. Of those that a mesh axis runs over, the one named last changes fastest.
Arguments:
- features: bfloat16 [1024, 512, 128], P('row', 'col'), may hold values from -6 to 6
- cotangent: bfloat16 [1024, 512, 128], P('row', 'col'), may hold values from -6 to 6
- kernels: bfloat16 [2, 9, 128, 128], replicated, may hold values from -0.1875 to 0.1875
- momentum: float32 [2, 147456], replicated, may hold values from -6 to 6
- mlp_in_weight: float32 [32, 3], replicated, may hold values from -3.5 to 3.5
- mlp_in_bias: float32 [32], replicated, may hold values from -3 to 3
- mlp_out_weight: float32 [2, 32], replicated, may hold values from -1 to 1
- mlp_out_bias: float32 [2], replicated, may hold values from -3 to 3
Outputs:
- update: float32 [2, 147456], replicated
- momentum_out: float32 [2, 147456], replicated
The draws below stay inside these ranges and needn't reach their ends.
All inputs are finite; a program needn't handle non-finite values.
Results may differ from the reference program's by a relative error of at most 0.0014.
Values may be sent and summed in bfloat16 or wider, within the bound.
No kernel may reach another device: no remote copies, remote signals or barrier semaphores. Data moves between devices by JAX's collectives and lax.ppermute only.
A program may use at most 64 MiB of HBM per device.

```python
import math
import jax
import jax.numpy as jnp
from jax import lax

C = 128
MLP_HID = 32
H = 1024
W = 512
KP = 147456


def block_levels(stream_key, shape, pieces, low, high):
    level = 1.0
    for axis_at, shards_of in pieces:
        heights = jax.random.uniform(jax.random.fold_in(jax.random.fold_in(stream_key, 6), axis_at), (shards_of,), jnp.float32, low / len(pieces), high / len(pieces))
        level = level * jnp.repeat(jnp.exp(heights), shape[axis_at] // shards_of).reshape((-1,) + (1,) * (len(shape) - 1 - axis_at))
    return level


def scatter_about(stream_key, shape, width, limit, shards=(), kind=jnp.bfloat16):
    entries = jax.random.normal(stream_key, shape, jnp.float32) * width
    if len(shards) > 0:
        entries = block_levels(stream_key, shape, shards, -0.22, 0.18) * entries
    return jnp.clip(entries, min=-limit, max=limit).astype(kind)


def setup_inputs(seed: int = 0) -> dict:
    key_of = jax.random.split(jax.random.key(seed), 9)
    features = scatter_about(key_of[0], (H, W, C), 1.0, 6.0, ((0, 16), (1, 16)))
    cotangent = scatter_about(key_of[1], (H, W, C), 1.0, 6.0, ((0, 16), (1, 16)))
    kernels = scatter_about(key_of[2], (2, 9, C, C), (9 * C) ** -0.5, 0.1875)
    momentum = scatter_about(key_of[3], (2, KP), 1.0, 6.0, (), jnp.float32)
    mlp_in_weight = scatter_about(key_of[4], (MLP_HID, 3), 3 ** -0.5, 3.5, (), jnp.float32)
    mlp_in_bias = scatter_about(key_of[5], (MLP_HID,), 0.5, 3.0, (), jnp.float32)
    mlp_out_weight = scatter_about(key_of[6], (2, MLP_HID), MLP_HID ** -0.5, 1.0, (), jnp.float32)
    mlp_out_bias = scatter_about(key_of[7], (2,), 0.5, 3.0, (), jnp.float32)
    return dict(features=features, cotangent=cotangent, kernels=kernels, momentum=momentum, mlp_in_weight=mlp_in_weight, mlp_in_bias=mlp_in_bias, mlp_out_weight=mlp_out_weight, mlp_out_bias=mlp_out_bias)


def convolve(image, kernel):
    summed = jnp.zeros((H * W, C), jnp.float32)
    for tap_row in range(3):
        for tap_col in range(3):
            moved = jnp.roll(image, (1 - tap_row, 1 - tap_col), axis=(0, 1)).reshape(H * W, C)
            summed = summed + jnp.dot(moved, kernel[3 * tap_row + tap_col], preferred_element_type=jnp.float32)
    return summed.reshape(H, W, C)

def kernel_grad(image, cotangent):
    flat_cot = cotangent.reshape(H * W, C)
    taps = []
    for tap_row in range(3):
        for tap_col in range(3):
            moved = jnp.roll(image, (1 - tap_row, 1 - tap_col), axis=(0, 1)).reshape(H * W, C)
            taps.append(lax.dot_general(moved, flat_cot, (((0,), (0,)), ((), ())), preferred_element_type=jnp.float32))
    return jnp.stack(taps)

def transpose_conv(cotangent, kernel):
    summed = jnp.zeros((H * W, C), jnp.float32)
    for tap_row in range(3):
        for tap_col in range(3):
            moved = jnp.roll(cotangent, (tap_row - 1, tap_col - 1), axis=(0, 1)).reshape(H * W, C)
            summed = summed + lax.dot_general(moved, kernel[3 * tap_row + tap_col], (((1,), (1,)), ((), ())), preferred_element_type=jnp.float32)
    return summed.reshape(H, W, C)

def learned_step(grads, squares, momentum, weights, w_in, b_in, w_out, b_out, gain, count):
    norm_scale = 1.0 / jnp.sqrt(squares / count + 1e-06)
    g_hat = grads * norm_scale[:, None]
    momentum_new = 0.9 * momentum + 0.1 * g_hat
    scaled = weights.astype(jnp.float32) * gain
    pre_units = w_in[:, 0][:, None, None] * g_hat[None] + w_in[:, 1][:, None, None] * momentum_new[None]
    pre_units = pre_units + w_in[:, 2][:, None, None] * scaled[None] + b_in[:, None, None]
    units = jax.nn.silu(pre_units)
    mlp_result = jnp.einsum('kh,hlp->klp', w_out, units, precision=lax.Precision.HIGHEST) + b_out[:, None, None]
    update = mlp_result[0] * jnp.exp(jnp.tanh(mlp_result[1]))
    return (update, momentum_new)

def reference(features, cotangent, kernels, momentum, mlp_in_weight, mlp_in_bias, mlp_out_weight, mlp_out_bias):
    pre_act = convolve(features, kernels[0])
    hidden = jax.nn.silu(pre_act).astype(jnp.bfloat16)
    grad_two = kernel_grad(hidden, cotangent)
    back_grad = transpose_conv(cotangent, kernels[1])
    sigma_val = jax.nn.sigmoid(pre_act)
    pre_grad = (back_grad * sigma_val * (1.0 + pre_act * (1.0 - sigma_val))).astype(jnp.bfloat16)
    grad_one = kernel_grad(features, pre_grad)
    grads = jnp.stack([grad_one.reshape(-1), grad_two.reshape(-1)])
    squares = lax.optimization_barrier(jnp.sum(grads * grads, axis=1))
    weights = kernels.reshape(2, KP)
    update, momentum_new = learned_step(grads, squares, momentum, weights, mlp_in_weight, mlp_in_bias, mlp_out_weight, mlp_out_bias, math.sqrt(9.0 * C), float(KP))
    return (update, momentum_new)
```

```python
import math

import jax
import jax.numpy as jnp
from jax import lax
from jax.sharding import PartitionSpec as P

AXES = ("row", "col")


def flat_index(x, y, z, core):
    return (((y % 2) * 4 + x) * 2 + core) * 16 + z * 2 + y // 2


COORDS = [(x, y, z, c) for y in range(4) for x in range(4) for z in range(8) for c in range(2)]


def pairs_of(fn):
    return [(flat_index(*p), flat_index(*fn(*p))) for p in COORDS]


CORE_PAIRS = pairs_of(lambda x, y, z, c: (x, y, z, 1 - c))
Z_TABLES = ((1, 0, 3, 2, 5, 4, 7, 6), (7, 2, 1, 4, 3, 6, 5, 0), (3, 6, 5, 0, 7, 2, 1, 4))
Z_PAIRS = [pairs_of(lambda x, y, z, c, t=t: (x, y, t[z], c)) for t in Z_TABLES]
PLANES = [
    [flat_index(x, y, z, c) for y in range(4) for x in range(4)] for z in range(8) for c in range(2)
]


def padded_2(cells, sides, width):
    for axis, dim in sides:
        count = lax.axis_size(axis)
        head = lax.slice_in_dim(cells, 0, width, axis=dim)
        tail = lax.slice_in_dim(cells, cells.shape[dim] - width, cells.shape[dim], axis=dim)
        cells = jnp.concatenate(
            [
                lax.ppermute(tail, axis, [(i, (i + 1) % count) for i in range(count)]),
                cells,
                lax.ppermute(head, axis, [((i + 1) % count, i) for i in range(count)]),
            ],
            axis=dim,
        )
    return cells


def window_of(padded, row, col, tile_rows, tile_cols):
    return padded[row : row + tile_rows, col : col + tile_cols].reshape(
        tile_rows * tile_cols, padded.shape[-1]
    )


def convolve(padded, kernel, tile_rows, tile_cols):
    summed = jnp.zeros((tile_rows * tile_cols, kernel.shape[-1]), jnp.float32)
    for tap in range(9):
        window = window_of(padded, tap // 3, tap % 3, tile_rows, tile_cols)
        summed = summed + jnp.dot(window, kernel[tap], preferred_element_type=jnp.float32)
    return summed


def transpose_conv(cot_pad, kernel, tile_rows, tile_cols):
    summed = jnp.zeros((tile_rows * tile_cols, kernel.shape[-2]), jnp.float32)
    for tap in range(9):
        window = window_of(cot_pad, 2 - tap // 3, 2 - tap % 3, tile_rows, tile_cols)
        summed = summed + lax.dot_general(
            window, kernel[tap], (((1,), (1,)), ((), ())), preferred_element_type=jnp.float32
        )
    return summed


def outer(left, right):
    return lax.dot_general(left, right, (((0,), (0,)), ((), ())), preferred_element_type=jnp.float32)


def on_device(
    features, cotangent, kernels, momentum, mlp_in_weight, mlp_in_bias, mlp_out_weight, mlp_out_bias
):
    tile_rows, tile_cols, channels = features.shape
    lines = 9 * channels
    core = lax.axis_index("row") % 2
    both = padded_2(jnp.stack([features, cotangent]), (("row", 1), ("col", 2)), 1)
    image_pad, cot_pad = both[0], both[1]
    pre_act = convolve(image_pad, kernels[0], tile_rows, tile_cols)
    hidden = jax.nn.silu(pre_act).astype(jnp.bfloat16)
    grad_two = jnp.concatenate(
        [
            outer(hidden, window_of(cot_pad, 2 - tap // 3, 2 - tap % 3, tile_rows, tile_cols))
            for tap in range(9)
        ]
    )
    back_grad = transpose_conv(cot_pad, kernels[1], tile_rows, tile_cols)
    sigma = jax.nn.sigmoid(pre_act)
    pre_grad = (back_grad * sigma * (1.0 + pre_act * (1.0 - sigma))).astype(jnp.bfloat16)
    grad_one = jnp.concatenate(
        [
            outer(window_of(image_pad, tap // 3, tap % 3, tile_rows, tile_cols), pre_grad)
            for tap in range(9)
        ]
    )
    first = core == 0
    mine = jnp.where(first, grad_one, grad_two)
    other = jnp.where(first, grad_two, grad_one)
    mine = mine + lax.ppermute(other, AXES, CORE_PAIRS)
    parts = lax.all_to_all(
        mine.reshape(16, lines // 16, channels), AXES, 0, 0, axis_index_groups=PLANES, tiled=True
    )
    part = jnp.sum(parts, axis=0)
    for pairs in Z_PAIRS:
        part = part + lax.ppermute(part, AXES, pairs)
    grads = lax.all_to_all(
        jnp.broadcast_to(part[None], parts.shape), AXES, 0, 0, axis_index_groups=PLANES, tiled=True
    ).reshape(lines, channels)

    count = float(lines * channels)
    pick = lambda a: jnp.where(first, a[0], a[1])
    scaled = pick(kernels.reshape(2, lines, channels)).astype(jnp.float32) * math.sqrt(9.0 * channels)
    g_hat = grads / jnp.sqrt(jnp.sum(grads * grads) / count + 1e-06)
    momentum_new = 0.9 * pick(momentum.reshape(2, lines, channels)) + 0.1 * g_hat
    top = jnp.zeros_like(g_hat)
    low = jnp.zeros_like(g_hat)
    for h in range(mlp_in_bias.shape[0]):
        pre = mlp_in_weight[h, 0] * g_hat + mlp_in_weight[h, 1] * momentum_new
        unit = jax.nn.silu(pre + mlp_in_weight[h, 2] * scaled + mlp_in_bias[h])
        top = top + mlp_out_weight[0, h] * unit
        low = low + mlp_out_weight[1, h] * unit
    update = (top + mlp_out_bias[0]) * jnp.exp(jnp.tanh(low + mlp_out_bias[1]))
    outs = []
    for value in (update, momentum_new):
        theirs = lax.ppermute(value, AXES, CORE_PAIRS)
        pair = jnp.stack([jnp.where(first, value, theirs), jnp.where(first, theirs, value)])
        outs.append(pair.reshape(2, lines * channels))
    return tuple(outs)


def solution(mesh):
    placed = (P("row", "col", None), P("row", "col", None), P(), P(), P(), P(), P(), P())
    return jax.shard_map(
        on_device, mesh=mesh, in_specs=placed, out_specs=(P(), P()), check_vma=False
    )
```

```python
import functools
import math

import jax
import jax.numpy as jnp
from jax import lax
from jax.experimental import pallas as pl
from jax.experimental.pallas import tpu as pltpu
from jax.sharding import PartitionSpec as P

AXES = ("row", "col")
BF16, F32 = jnp.bfloat16, jnp.float32
ROWS, COLS, CH = 64, 32, 128
CELLS = ROWS * COLS
PADDED = (ROWS + 2) * COLS
LINES = 9 * CH
EDGE = 80
HID = 32


def flat_index(x, y, z, core):
    return (((y % 2) * 4 + x) * 2 + core) * 16 + z * 2 + y // 2


COORDS = [(x, y, z, c) for y in range(4) for x in range(4) for z in range(8) for c in range(2)]


def pairs_of(fn):
    return [(flat_index(*p), flat_index(*fn(*p))) for p in COORDS]


CORE_PAIRS = pairs_of(lambda x, y, z, c: (x, y, z, 1 - c))
Z_TABLES = ((1, 0, 3, 2, 5, 4, 7, 6), (7, 2, 1, 4, 3, 6, 5, 0), (3, 6, 5, 0, 7, 2, 1, 4))
Z_PAIRS = [pairs_of(lambda x, y, z, c, t=t: (x, y, t[z], c)) for t in Z_TABLES]
PLANES = [
    [flat_index(x, y, z, c) for y in range(4) for x in range(4)] for z in range(8) for c in range(2)
]
VMEM = pl.BlockSpec(memory_space=pltpu.VMEM)
SMEM = pl.BlockSpec(memory_space=pltpu.SMEM)


def shape(dims, dtype):
    return jax.ShapeDtypeStruct(dims, dtype)


def call(body, ins, outs, micros, scratch=(), aliases=None):
    return pl.pallas_call(
        body,
        out_shape=outs,
        in_specs=ins,
        out_specs=jax.tree.map(lambda _: VMEM, outs),
        scratch_shapes=list(scratch),
        input_output_aliases=aliases or {},
        compiler_params=pltpu.CompilerParams(vmem_limit_bytes=40 * 1024 * 1024),
        cost_estimate=pl.CostEstimate(
            flops=int(micros * 8e6), bytes_accessed=1024, transcendentals=0
        ),
    )


def dot(left, right, over):
    return lax.dot_general(left, right, (over, ((), ())), preferred_element_type=F32)


def edges_body(image_ref, cot_ref, first_ref, last_ref):
    for at, ref in enumerate((image_ref, cot_ref)):
        head = ref[:, 0:16, :].astype(F32)
        tail = ref[:, 16:32, :].astype(F32)
        first_ref[at, 8:72, :] = head[:, 0, :]
        last_ref[at, 8:72, :] = tail[:, 15, :]


def corners_body(first_ref, last_ref, above_ref, below_ref, send_first_ref, send_last_ref):
    for at in range(2):
        above = above_ref[at].astype(F32)
        below = below_ref[at].astype(F32)
        for src, dst, col in ((first_ref, send_first_ref, 0), (last_ref, send_last_ref, 31)):
            line = lax.broadcasted_iota(jnp.int32, (8, CH), 0)
            top = jnp.where(line == 7, jnp.broadcast_to(above[col : col + 1], (8, CH)), 0.0)
            low = jnp.where(line == 0, jnp.broadcast_to(below[col : col + 1], (8, CH)), 0.0)
            dst[at] = jnp.concatenate([top, src[at, 8:72, :], low], axis=0).astype(BF16)


def taps_of(ref, start, count):
    return jnp.concatenate([ref[start + a * COLS : start + a * COLS + count, :] for a in range(3)], axis=1)


def back_weights(k_ref, taps):
    return jnp.concatenate([k_ref[1, tap] for tap in taps], axis=1)


def inner_body(image_ref, cot_ref, above_ref, below_ref, k_ref, x3_ref, c3_ref, pre_ref, back_ref, flat_ref):
    for at, (ref, out_ref) in enumerate(((image_ref, x3_ref), (cot_ref, c3_ref))):
        out_ref[0:COLS, CH : 2 * CH] = above_ref[at]
        out_ref[COLS : COLS + CELLS, CH : 2 * CH] = ref[...].reshape(CELLS, CH)
        out_ref[COLS + CELLS :, CH : 2 * CH] = below_ref[at]
        flat_ref[8 : 8 + COLS, :] = above_ref[at].astype(F32)
        flat_ref[8 + COLS : 8 + COLS + CELLS, :] = ref[...].reshape(CELLS, CH).astype(F32)
        flat_ref[8 + COLS + CELLS : 8 + PADDED, :] = below_ref[at].astype(F32)
        step = 6 * COLS
        col = lax.broadcasted_iota(jnp.int32, (step, CH), 0) % COLS
        for start in range(0, PADDED, step):
            early = jnp.where(col == 0, 0.0, flat_ref[7 + start : 7 + start + step, :])
            late = jnp.where(col == COLS - 1, 0.0, flat_ref[9 + start : 9 + start + step, :])
            out_ref[start : start + step, 0:CH] = early.astype(BF16)
            out_ref[start : start + step, 2 * CH :] = late.astype(BF16)
    size = 512
    forward = k_ref[0].reshape(LINES, CH)
    backward = back_weights(k_ref, range(8, -1, -1))
    for start in range(0, CELLS, size):
        pre_ref[start : start + size, :] = dot(taps_of(x3_ref, start, size), forward, ((1,), (0,)))
        back_ref[start : start + size, :] = dot(taps_of(c3_ref, start, size), backward, ((1,), (1,)))


def outer_body(
    x3_ref, c3_ref, pre_ref, back_ref, left_ref, right_ref, k_ref,
    x3_out, c3_out, hidden_ref, pre_grad_ref, edge_ref, mid_ref, grad_ref,
):
    mid_ref[...] = pre_ref[...]
    grad_ref[...] = back_ref[...]
    for at in range(2):
        out_ref = (x3_out, c3_out)[at]
        total_ref = (mid_ref, grad_ref)[at]
        for side, (ref, col, lane) in enumerate(((left_ref, 0, 0), (right_ref, COLS - 1, 2 * CH))):
            slot = 2 * at + side
            edge_ref[slot] = ref[at].astype(F32)
            lines = jnp.concatenate([edge_ref[slot, 7 + a : 71 + a, :] for a in range(3)], axis=1).astype(BF16)
            if at == 0:
                weights = jnp.concatenate([k_ref[0, 3 * a + 2 * side] for a in range(3)], axis=0)
                extra = dot(lines, weights, ((1,), (0,)))
            else:
                extra = dot(lines, back_weights(k_ref, [8 - 3 * a - 2 * side for a in range(3)]), ((1,), (1,)))
            spots = pl.ds(col, ROWS, stride=COLS)
            total_ref[spots, :] = total_ref[spots, :] + extra
            line = lax.broadcasted_iota(jnp.int32, (16, CH), 0)
            for r in range(ROWS + 2):
                base = r * COLS + (col // 16) * 16
                old = out_ref[base : base + 16, lane : lane + CH].astype(F32)
                new = jnp.broadcast_to(edge_ref[slot, 7 + r : 8 + r, :], (16, CH))
                out_ref[base : base + 16, lane : lane + CH] = jnp.where(line == col % 16, new, old).astype(BF16)
    size = 128
    for start in range(0, CELLS, size):
        mid = mid_ref[start : start + size, :]
        sigma = jax.nn.sigmoid(mid)
        hidden_ref[start : start + size, :] = (mid * sigma).astype(BF16)
        grad = grad_ref[start : start + size, :] * sigma * (1.0 + mid * (1.0 - sigma))
        pre_grad_ref[start : start + size, :] = grad.astype(BF16)


def grads_body(flip, core_ref, hidden_ref, pre_grad_ref, x3_ref, c3_ref, out_ref):
    which = core_ref[0] if flip == 0 else 1 - core_ref[0]

    @pl.when(which == 0)
    def _():
        left = pre_grad_ref[...]
        for a in range(3):
            part = dot(left, x3_ref[a * COLS : a * COLS + CELLS, :], ((0,), (0,)))
            for b in range(3):
                tap = 3 * a + b
                out_ref[tap * CH : (tap + 1) * CH, :] = part[:, b * CH : (b + 1) * CH].T

    @pl.when(which == 1)
    def _():
        left = hidden_ref[...]
        for a in range(3):
            part = dot(left, c3_ref[a * COLS : a * COLS + CELLS, :], ((0,), (0,)))
            for b in range(3):
                tap = 8 - 3 * a - b
                out_ref[tap * CH : (tap + 1) * CH, :] = part[:, b * CH : (b + 1) * CH]


def add_body(left_ref, right_ref, out_ref):
    out_ref[...] = left_ref[...] + right_ref[...]


def fold_body(parts_ref, out_ref):
    total = parts_ref[0]
    for i in range(1, 16):
        total = total + parts_ref[i]
    out_ref[...] = total


def momentum_body(core_ref, grads_ref, momentum_ref, out_ref, scale_ref):
    total = jnp.zeros((8, CH), F32)
    for i in range(16):
        part = grads_ref[i]
        total = total + jnp.sum((part * part).reshape(9, 8, CH), axis=0)
    squares = jnp.sum(total)
    scale = 1.0 / jnp.sqrt(jnp.full((8, CH), squares, F32) / float(LINES * CH) + 1e-06)
    scale_ref[...] = scale
    line = jnp.broadcast_to(scale[0:1], (72, CH))
    for layer in range(2):

        @pl.when(core_ref[0] == layer)
        def _():
            for i in range(16):
                old = momentum_ref[pl.ds(2 * 72 * i + layer, 72, stride=2), :]
                out_ref[i * 72 : (i + 1) * 72, :] = 0.9 * old + 0.1 * (grads_ref[i] * line)


def mlp_body(core_ref, w_ref, b_ref, v_ref, c_ref, grads_ref, new_ref, scale_ref, k_ref, out_ref):
    block = 48
    gain = math.sqrt(9.0 * CH)
    scale = jnp.broadcast_to(scale_ref[0:1], (block, CH))
    base = core_ref[0] * LINES

    def step(i, _):
        rows = pl.ds(pl.multiple_of(i * block, block), block)
        g_hat = grads_ref[rows, :] * scale
        new = new_ref[rows, :]
        scaled = k_ref[pl.ds(pl.multiple_of(base + i * block, 16), block), :].astype(F32) * gain
        top = jnp.full((block, CH), c_ref[0], F32)
        low = jnp.full((block, CH), c_ref[1], F32)
        for h in range(HID):
            half = (0.5 * w_ref[h, 0]) * g_hat + (0.5 * w_ref[h, 1]) * new
            half = half + (0.5 * w_ref[h, 2]) * scaled + 0.5 * b_ref[h]
            unit = half + half * jnp.tanh(half)
            top = top + v_ref[0, h] * unit
            low = low + v_ref[1, h] * unit
        out_ref[rows, :] = top * jnp.exp(jnp.tanh(low))
        return 0

    lax.fori_loop(0, LINES // block, step, 0)


def weave_body(core_ref, mine_ref, theirs_ref, out_ref):
    for layer in range(2):

        @pl.when(core_ref[0] == layer)
        def _():
            for start in range(0, LINES, 72):
                out_ref[pl.ds(2 * start + layer, 72, stride=2), :] = mine_ref[start : start + 72, :]
                out_ref[pl.ds(2 * start + 1 - layer, 72, stride=2), :] = theirs_ref[start : start + 72, :]


def on_device(
    features, cotangent, kernels, momentum, mlp_in_weight, mlp_in_bias, mlp_out_weight, mlp_out_bias
):
    core = (lax.axis_index("row") % 2).astype(jnp.int32).reshape(1)
    count_r, count_c = lax.axis_size("row"), lax.axis_size("col")
    up = lambda n: [(i, (i + 1) % n) for i in range(n)]
    down = lambda n: [((i + 1) % n, i) for i in range(n)]

    above = lax.ppermute(jnp.stack([features[-1], cotangent[-1]]), "row", up(count_r))
    below = lax.ppermute(jnp.stack([features[0], cotangent[0]]), "row", down(count_r))
    columns = (shape((2, EDGE, CH), F32),) * 2
    first, last = call(edges_body, [VMEM] * 2, columns, 0.5)(features, cotangent)
    columns = (shape((2, EDGE, CH), BF16),) * 2
    first, last = call(corners_body, [VMEM] * 4, columns, 0.2)(first, last, above, below)
    left = lax.ppermute(last, "col", up(count_c))
    right = lax.ppermute(first, "col", down(count_c))
    wide, tile = shape((PADDED, 3 * CH), BF16), shape((CELLS, CH), F32)
    x3, c3, pre, back = call(
        inner_body, [VMEM] * 5, (wide, wide, tile, tile), 5.0, [pltpu.VMEM((PADDED + 16, CH), F32)]
    )(features, cotangent, above, below, kernels)
    narrow = shape((CELLS, CH), BF16)
    x3, c3, hidden, pre_grad = call(
        outer_body,
        [VMEM] * 7,
        (wide, wide, narrow, narrow),
        1.5,
        [pltpu.VMEM((4, EDGE, CH), F32), pltpu.VMEM((CELLS, CH), F32), pltpu.VMEM((CELLS, CH), F32)],
        {0: 0, 1: 1},
    )(x3, c3, pre, back, left, right, kernels)

    layer = shape((LINES, CH), F32)
    gradient = lambda flip: call(functools.partial(grads_body, flip), [SMEM] + [VMEM] * 4, layer, 2.5)(
        core, hidden, pre_grad, x3, c3
    )
    theirs = lax.ppermute(gradient(1), AXES, CORE_PAIRS)
    mine = call(add_body, [VMEM] * 2, layer, 0.3)(gradient(0), theirs)
    parts = lax.all_to_all(
        mine.reshape(16, LINES // 16, CH), AXES, 0, 0, axis_index_groups=PLANES, tiled=True
    )
    part = call(fold_body, [VMEM], shape((LINES // 16, CH), F32), 0.3)(parts)
    for pairs in Z_PAIRS:
        part = part + lax.ppermute(part, AXES, pairs)
    grads = lax.all_to_all(
        jnp.broadcast_to(part[None], parts.shape), AXES, 0, 0, axis_index_groups=PLANES, tiled=True
    )

    woven = momentum.reshape(2, LINES, CH).transpose(1, 0, 2).reshape(2 * LINES, CH)
    new, scale = call(momentum_body, [SMEM, VMEM, VMEM], (layer, shape((8, CH), F32)), 0.5)(
        core, grads, woven
    )
    new_theirs = lax.ppermute(new, AXES, CORE_PAIRS)
    update = call(mlp_body, [SMEM] * 5 + [VMEM] * 4, layer, 8.0)(
        core, mlp_in_weight, mlp_in_bias, mlp_out_weight, mlp_out_bias,
        grads.reshape(LINES, CH), new, scale, kernels.reshape(2 * LINES, CH),
    )
    update_theirs = lax.ppermute(update, AXES, CORE_PAIRS)
    outs = []
    for own, other in ((update, update_theirs), (new, new_theirs)):
        both = call(weave_body, [SMEM] + [VMEM] * 2, shape((2 * LINES, CH), F32), 0.5)(core, own, other)
        outs.append(both.reshape(LINES, 2, CH).transpose(1, 0, 2).reshape(2, LINES * CH))
    return tuple(outs)


def solution(mesh):
    placed = (P("row", "col", None), P("row", "col", None), P(), P(), P(), P(), P(), P())
    return jax.shard_map(
        on_device, mesh=mesh, in_specs=placed, out_specs=(P(), P()), check_vma=False
    )
```

```python
import functools
import math

import jax
import jax.numpy as jnp
from jax import lax
from jax.experimental import pallas as pl
from jax.experimental.pallas import tpu as pltpu
from jax.sharding import PartitionSpec as P

AXES = ("row", "col")
BF16, F32 = jnp.bfloat16, jnp.float32
ROWS, COLS, CH = 64, 32, 128
CELLS = ROWS * COLS
PADDED = (ROWS + 2) * COLS
LINES = 9 * CH
EDGE = 80
HID = 32


def flat_index(x, y, z, core):
    return (((y % 2) * 4 + x) * 2 + core) * 16 + z * 2 + y // 2


COORDS = [(x, y, z, c) for y in range(4) for x in range(4) for z in range(8) for c in range(2)]


def pairs_of(fn):
    return [(flat_index(*p), flat_index(*fn(*p))) for p in COORDS]


CORE_PAIRS = pairs_of(lambda x, y, z, c: (x, y, z, 1 - c))
Z_PAIRS = [
    pairs_of(lambda x, y, z, c, fn=fn: (x, y, fn(z) % 8, c))
    for fn in (
        lambda z: z ^ 1,
        lambda z: z + 1 if z % 2 else z - 1,
        lambda z: z + 2 if z % 2 else z - 2,
        lambda z: z - 3 if z % 2 == 0 else z + 3,
    )
]


def turn(x, y, z, c, along_x, k):
    return ((x + k) % 4, y, z, c) if along_x else (x, (y + k) % 4, z, c)


FIRST_PAIRS = [pairs_of(lambda x, y, z, c, k=k: turn(x, y, z, c, c == 0, k)) for k in (1, 3, 2)]
SECOND_PAIRS = [pairs_of(lambda x, y, z, c, k=k: turn(x, y, z, c, c == 1, k)) for k in (1, 3, 2)]
TURNS = (1, 3, 2)
PLANES = [
    [flat_index(*((i // 4, i % 4) if c == 0 else (i % 4, i // 4)), z, c) for i in range(16)]
    for z in range(8)
    for c in range(2)
]
VMEM = pl.BlockSpec(memory_space=pltpu.VMEM)
SMEM = pl.BlockSpec(memory_space=pltpu.SMEM)


HBM = pl.BlockSpec(memory_space=pltpu.HBM)


def place():
    row, col = lax.axis_index("row"), lax.axis_index("col")
    core, x, y, z = row & 1, (row >> 1) & 3, (col & 1) * 2 + (row >> 3), col >> 1
    first = jnp.where(core == 0, x, y)
    return core, first, x + y - first, z


def shape(dims, dtype):
    return jax.ShapeDtypeStruct(dims, dtype)


def call(body, ins, outs, micros, scratch=(), aliases=None):
    return pl.pallas_call(
        body,
        out_shape=outs,
        in_specs=ins,
        out_specs=jax.tree.map(lambda _: VMEM, outs),
        scratch_shapes=list(scratch),
        input_output_aliases=aliases or {},
        compiler_params=pltpu.CompilerParams(vmem_limit_bytes=20 * 1024 * 1024),
        cost_estimate=pl.CostEstimate(
            flops=int(micros * 8e6), bytes_accessed=1024, transcendentals=0
        ),
    )


def dot(left, right, over):
    return lax.dot_general(left, right, (over, ((), ())), preferred_element_type=F32)


def edges_body(image_ref, cot_ref, image_out, cot_out, top_ref, low_ref, first_ref, last_ref, sem):
    pairs = ((image_ref, image_out), (cot_ref, cot_out))
    copies = [pltpu.make_async_copy(src, dst, sem.at[at]) for at, (src, dst) in enumerate(pairs)]
    for copy in copies:
        copy.start()
    for at, ref in enumerate((image_out, cot_out)):
        copies[at].wait()
        top_ref[at] = ref[0]
        low_ref[at] = ref[ROWS - 1]
        first_ref[at, 8:72, :] = ref[:, 0:16, :].astype(F32)[:, 0, :]
        last_ref[at, 8:72, :] = ref[:, COLS - 16 : COLS, :].astype(F32)[:, 15, :]


def corners_body(first_ref, last_ref, above_ref, below_ref, send_first_ref, send_last_ref):
    for at in range(2):
        above = above_ref[at].astype(F32)
        below = below_ref[at].astype(F32)
        for src, dst, col in ((first_ref, send_first_ref, 0), (last_ref, send_last_ref, 31)):
            line = lax.broadcasted_iota(jnp.int32, (8, CH), 0)
            top = jnp.where(line == 7, jnp.broadcast_to(above[col : col + 1], (8, CH)), 0.0)
            low = jnp.where(line == 0, jnp.broadcast_to(below[col : col + 1], (8, CH)), 0.0)
            dst[at] = jnp.concatenate([top, src[at, 8:72, :], low], axis=0).astype(BF16)


def taps_of(ref, start, count):
    return jnp.concatenate([ref[start + a * COLS : start + a * COLS + count, :] for a in range(3)], axis=1)


def back_weights(k_ref, taps):
    return jnp.concatenate([k_ref[1, tap] for tap in taps], axis=1)


def inner_body(image_ref, cot_ref, above_ref, below_ref, k_ref, x3_ref, c3_ref, pre_ref, back_ref, flat_ref):
    for at, (ref, out_ref) in enumerate(((image_ref, x3_ref), (cot_ref, c3_ref))):
        out_ref[0:COLS, CH : 2 * CH] = above_ref[at]
        out_ref[COLS : COLS + CELLS, CH : 2 * CH] = ref[...].reshape(CELLS, CH)
        out_ref[COLS + CELLS :, CH : 2 * CH] = below_ref[at]
        flat_ref[8 : 8 + COLS, :] = above_ref[at].astype(F32)
        flat_ref[8 + COLS : 8 + COLS + CELLS, :] = ref[...].reshape(CELLS, CH).astype(F32)
        flat_ref[8 + COLS + CELLS : 8 + PADDED, :] = below_ref[at].astype(F32)
        step = 6 * COLS
        col = lax.broadcasted_iota(jnp.int32, (step, CH), 0) % COLS
        for start in range(0, PADDED, step):
            early = jnp.where(col == 0, 0.0, flat_ref[7 + start : 7 + start + step, :])
            late = jnp.where(col == COLS - 1, 0.0, flat_ref[9 + start : 9 + start + step, :])
            out_ref[start : start + step, 0:CH] = early.astype(BF16)
            out_ref[start : start + step, 2 * CH :] = late.astype(BF16)
    size = 512
    forward = k_ref[0].reshape(LINES, CH)
    backward = back_weights(k_ref, range(8, -1, -1))
    for start in range(0, CELLS, size):
        pre_ref[start : start + size, :] = dot(taps_of(x3_ref, start, size), forward, ((1,), (0,)))
        back_ref[start : start + size, :] = dot(taps_of(c3_ref, start, size), backward, ((1,), (1,)))


def outer_body(
    x3_ref, c3_ref, pre_ref, back_ref, left_ref, right_ref, k_ref,
    x3_out, c3_out, hidden_ref, pre_grad_ref, edge_ref, mid_ref, grad_ref,
):
    mid_ref[...] = pre_ref[...]
    grad_ref[...] = back_ref[...]
    for at in range(2):
        out_ref = (x3_out, c3_out)[at]
        total_ref = (mid_ref, grad_ref)[at]
        for side, (ref, col, lane) in enumerate(((left_ref, 0, 0), (right_ref, COLS - 1, 2 * CH))):
            slot = 2 * at + side
            edge_ref[slot] = ref[at].astype(F32)
            lines = jnp.concatenate([edge_ref[slot, 7 + a : 71 + a, :] for a in range(3)], axis=1).astype(BF16)
            if at == 0:
                weights = jnp.concatenate([k_ref[0, 3 * a + 2 * side] for a in range(3)], axis=0)
                extra = dot(lines, weights, ((1,), (0,)))
            else:
                extra = dot(lines, back_weights(k_ref, [8 - 3 * a - 2 * side for a in range(3)]), ((1,), (1,)))
            spots = pl.ds(col, ROWS, stride=COLS)
            total_ref[spots, :] = total_ref[spots, :] + extra
            line = lax.broadcasted_iota(jnp.int32, (16, CH), 0)
            for r in range(ROWS + 2):
                base = r * COLS + (col // 16) * 16
                old = out_ref[base : base + 16, lane : lane + CH].astype(F32)
                new = jnp.broadcast_to(edge_ref[slot, 7 + r : 8 + r, :], (16, CH))
                out_ref[base : base + 16, lane : lane + CH] = jnp.where(line == col % 16, new, old).astype(BF16)
    size = 128
    for start in range(0, CELLS, size):
        mid = mid_ref[start : start + size, :]
        sigma = jax.nn.sigmoid(mid)
        hidden_ref[start : start + size, :] = (mid * sigma).astype(BF16)
        grad = grad_ref[start : start + size, :] * sigma * (1.0 + mid * (1.0 - sigma))
        pre_grad_ref[start : start + size, :] = grad.astype(BF16)


def grads_body(flip, hidden_ref, pre_grad_ref, x3_ref, c3_ref, out_ref):
    core = place()[0]
    which = core if flip == 0 else 1 - core

    @pl.when(which == 0)
    def _():
        left = pre_grad_ref[...]
        for a in range(3):
            part = dot(left, x3_ref[a * COLS : a * COLS + CELLS, :], ((0,), (0,)))
            for b in range(3):
                tap = 3 * a + b
                out_ref[tap * CH : (tap + 1) * CH, :] = part[:, b * CH : (b + 1) * CH].T

    @pl.when(which == 1)
    def _():
        left = hidden_ref[...]
        for a in range(3):
            part = dot(left, c3_ref[a * COLS : a * COLS + CELLS, :], ((0,), (0,)))
            for b in range(3):
                tap = 8 - 3 * a - b
                out_ref[tap * CH : (tap + 1) * CH, :] = part[:, b * CH : (b + 1) * CH]


def deal(value_of, at, size, outs):
    for turn_by, out_ref in zip((0,) + TURNS, outs):
        start = pl.multiple_of(((at + turn_by) & 3) * size, 8)
        out_ref[...] = value_of(pl.ds(start, size))


def add_body(left_ref, right_ref, *outs):
    deal(lambda rows: left_ref[rows, :] + right_ref[rows, :], place()[1], LINES // 4, outs)


def fold_body(own_ref, a_ref, b_ref, c_ref, *outs):
    def value_of(rows):
        return (own_ref[rows, :] + a_ref[rows, :]) + (b_ref[rows, :] + c_ref[rows, :])

    deal(value_of, place()[2], LINES // 16, outs)


def last_fold_body(own_ref, a_ref, b_ref, c_ref, out_ref):
    out_ref[...] = (own_ref[...] + a_ref[...]) + (b_ref[...] + c_ref[...])


def last_pair_body(left_ref, right_ref, out_ref):
    out_ref[...] = left_ref[...] + right_ref[...]


def finish_body(own_ref, near_ref, far_ref, across_ref, out_ref):
    total = (own_ref[...] + across_ref[...]) + (near_ref[...] + far_ref[...])
    for i in range(16):
        out_ref[i] = total


def momentum_body(grads_ref, momentum_ref, out_ref, scale_ref):
    core = place()[0]
    total = jnp.zeros((8, CH), F32)
    for start in range(0, LINES, 72):
        part = grads_ref[start : start + 72, :]
        total = total + jnp.sum((part * part).reshape(9, 8, CH), axis=0)
    squares = jnp.sum(total)
    scale = 1.0 / jnp.sqrt(jnp.full((8, CH), squares, F32) / float(LINES * CH) + 1e-06)
    scale_ref[...] = scale
    line = jnp.broadcast_to(scale[0:1], (72, CH))
    for layer in range(2):

        @pl.when(core == layer)
        def _():
            for start in range(0, LINES, 72):
                old = momentum_ref[pl.ds(2 * start + layer, 72, stride=2), :]
                out_ref[start : start + 72, :] = 0.9 * old + 0.1 * (grads_ref[start : start + 72, :] * line)


PIECES = 9
DEPTH = 80
OUTS = 8 * (HID + 2)


def table_body(spread_ref, out_ref):
    row = lax.broadcasted_iota(jnp.int32, (OUTS, CH), 0) % 8
    lane = lax.broadcasted_iota(jnp.int32, (OUTS, CH), 1)
    same = row == lane % 8
    total = jnp.zeros((OUTS, CH), F32)
    for term in range(4):
        value = jnp.broadcast_to(spread_ref[:, term : term + 1], (OUTS, CH))
        high = value.astype(BF16).astype(F32)
        low = value - high
        if term == 3:
            total = jnp.where(lane == 64, high, jnp.where(lane == 65, low, total))
        else:
            slots = ((high, 3 * term), (high, 3 * term + 1), (low, 3 * term + 2)) if term < 2 else ((high, 6), (low, 7))
            for part, piece in slots:
                total = jnp.where(same & (lane // 8 == piece), part, total)
    out_ref[...] = total.astype(BF16)


def mlp_body(v_ref, table_ref, grads_ref, new_ref, scale_ref, k_ref, out_ref):
    block, blocks = 64, 6
    scale = jnp.broadcast_to(scale_ref[0:1], (block, CH))
    base = place()[0] * LINES
    table = table_ref[:, 0:DEPTH]

    def wide(value):
        return jnp.concatenate([value[8 * j : 8 * j + 8] for j in range(block // 8)], axis=1)

    def one(start):
        rows = pl.ds(pl.multiple_of(start, block), block)
        parts = []
        for value in (grads_ref[rows, :] * scale, new_ref[rows, :]):
            high = value.astype(BF16).astype(F32)
            parts += [wide(high), wide(value - high), wide(high)]
        scaled = wide(k_ref[pl.ds(pl.multiple_of(base + start, block), block), :].astype(F32))
        ones = jnp.ones_like(scaled)
        inputs = jnp.concatenate(parts + [scaled, scaled, ones, ones], axis=0).astype(BF16)
        halves = dot(table, inputs, ((1,), (0,)))
        top = halves[8 * HID : 8 * HID + 8]
        low = halves[8 * HID + 8 : 8 * HID + 16]
        for h in range(HID):
            half = halves[8 * h : 8 * h + 8]
            curved = half * jnp.tanh(half)
            top = top + v_ref[0, h] * curved
            low = low + v_ref[1, h] * curved
        value = top * jnp.exp(jnp.tanh(low))
        for j in range(block // 8):
            out_ref[pl.ds(pl.multiple_of(start + 8 * j, 8), 8), :] = value[:, j * CH : (j + 1) * CH]

    def step(i, _):
        for j in range(blocks):
            one((i * blocks + j) * block)
        return 0

    lax.fori_loop(0, LINES // (block * blocks), step, 0)


def weave_body(mine_ref, theirs_ref, out_ref):
    core = place()[0]
    for layer in range(2):

        @pl.when(core == layer)
        def _():
            for start in range(0, LINES, 72):
                out_ref[pl.ds(2 * start + layer, 72, stride=2), :] = mine_ref[start : start + 72, :]
                out_ref[pl.ds(2 * start + 1 - layer, 72, stride=2), :] = theirs_ref[start : start + 72, :]


def on_device(
    features, cotangent, kernels, momentum, mlp_in_weight, mlp_in_bias, mlp_out_weight, mlp_out_bias
):
    count_r, count_c = lax.axis_size("row"), lax.axis_size("col")
    up = lambda n: [(i, (i + 1) % n) for i in range(n)]
    down = lambda n: [((i + 1) % n, i) for i in range(n)]

    line, column = shape((2, COLS, CH), BF16), shape((2, EDGE, CH), F32)
    whole = shape((ROWS, COLS, CH), BF16)
    features, cotangent, top, low, first, last = call(
        edges_body,
        [HBM] * 2,
        (whole, whole, line, line, column, column),
        1.5,
        [pltpu.SemaphoreType.DMA((2,))],
    )(features, cotangent)
    above = lax.ppermute(low, "row", up(count_r))
    below = lax.ppermute(top, "row", down(count_r))
    columns = (shape((2, EDGE, CH), BF16),) * 2
    first, last = call(corners_body, [VMEM] * 4, columns, 0.2)(first, last, above, below)
    left = lax.ppermute(last, "col", up(count_c))
    right = lax.ppermute(first, "col", down(count_c))
    wide, tile = shape((PADDED, 3 * CH), BF16), shape((CELLS, CH), F32)
    x3, c3, pre, back = call(
        inner_body, [VMEM] * 5, (wide, wide, tile, tile), 5.0, [pltpu.VMEM((PADDED + 16, CH), F32)]
    )(features, cotangent, above, below, kernels)
    narrow = shape((CELLS, CH), BF16)
    x3, c3, hidden, pre_grad = call(
        outer_body,
        [VMEM] * 7,
        (wide, wide, narrow, narrow),
        1.5,
        [pltpu.VMEM((4, EDGE, CH), F32), pltpu.VMEM((CELLS, CH), F32), pltpu.VMEM((CELLS, CH), F32)],
        {0: 0, 1: 1},
    )(x3, c3, pre, back, left, right, kernels)

    layer = shape((LINES, CH), F32)
    gradient = lambda flip: call(functools.partial(grads_body, flip), [VMEM] * 4, layer, 1.5)(
        hidden, pre_grad, x3, c3
    )
    theirs = lax.ppermute(gradient(1), AXES, CORE_PAIRS)
    quarter, part = shape((LINES // 4, CH), F32), shape((LINES // 16, CH), F32)
    own, *sent = call(add_body, [VMEM] * 2, (quarter,) * 4, 0.3)(gradient(0), theirs)
    got = [lax.ppermute(s, AXES, pairs) for s, pairs in zip(sent, FIRST_PAIRS)]
    own, *sent = call(fold_body, [VMEM] * 4, (part,) * 4, 0.3)(own, *got)
    got = [lax.ppermute(s, AXES, pairs) for s, pairs in zip(sent, SECOND_PAIRS)]
    own = call(last_fold_body, [VMEM] * 4, part, 0.2)(own, *got)
    own = call(last_pair_body, [VMEM] * 2, part, 0.2)(own, lax.ppermute(own, AXES, Z_PAIRS[0]))
    got = [lax.ppermute(own, AXES, pairs) for pairs in Z_PAIRS[1:]]
    copies = call(finish_body, [VMEM] * 4, shape((16, LINES // 16, CH), F32), 0.2)(own, *got)
    grads = lax.all_to_all(copies, AXES, 0, 0, axis_index_groups=PLANES, tiled=True)
    grads = grads.reshape(LINES, CH)

    woven = momentum.reshape(2, LINES, CH).transpose(1, 0, 2).reshape(2 * LINES, CH)
    new, scale = call(momentum_body, [VMEM] * 2, (layer, shape((8, CH), F32)), 0.5)(grads, woven)
    new_theirs = lax.ppermute(new, AXES, CORE_PAIRS)
    gain = jnp.array([1.0, 1.0, math.sqrt(9.0 * CH), 1.0], F32)
    terms = 0.5 * jnp.concatenate([mlp_in_weight, mlp_in_bias[:, None]], axis=1) * gain
    linear = jnp.sum(mlp_out_weight[:, :, None] * terms[None], axis=1)
    linear = linear + jnp.pad(mlp_out_bias[:, None], ((0, 0), (3, 0)))
    spread = jnp.repeat(jnp.concatenate([terms, linear]), 8, axis=0)
    table = call(table_body, [VMEM], shape((OUTS, CH), BF16), 0.5)(spread)
    update = call(
        mlp_body, [SMEM] + [VMEM] * 5, layer, 5.0
    )(mlp_out_weight, table, grads, new, scale, kernels.reshape(2 * LINES, CH))
    update_theirs = lax.ppermute(update, AXES, CORE_PAIRS)
    outs = []
    for mine, other in ((update, update_theirs), (new, new_theirs)):
        both = call(weave_body, [VMEM] * 2, shape((2 * LINES, CH), F32), 0.5)(mine, other)
        outs.append(both.reshape(LINES, 2, CH).transpose(1, 0, 2).reshape(2, LINES * CH))
    return tuple(outs)


def solution(mesh):
    placed = (P("row", "col", None), P("row", "col", None), P(), P(), P(), P(), P(), P())
    return jax.shard_map(
        on_device, mesh=mesh, in_specs=placed, out_specs=(P(), P()), check_vma=False
    )
```
